32 devices in a mesh: shard: 4 (over y, x), cols: 8 (over z, core).
Axes of the slice: x: 2, y: 2, z: 4, core: 2. Of those that a mesh axis runs over, the one named last changes fastest.
Arguments:
- train_gate: bfloat16 [4096, 14336], P('shard', 'cols'), may hold values from -0.09375 to 0.09375
- low_gate: bfloat16 [4096, 32], P('shard'), may hold values from -0.09375 to 0.09375
- high_gate: bfloat16 [32, 14336], P(None, 'cols'), may hold values from -1 to 1
- train_up: bfloat16 [4096, 14336], P('shard', 'cols'), may hold values from -0.09375 to 0.09375
- low_up: bfloat16 [4096, 32], P('shard'), may hold values from -0.09375 to 0.09375
- high_up: bfloat16 [32, 14336], P(None, 'cols'), may hold values from -1 to 1
- norm_train: float32 [4096], P(('shard', 'cols')), may hold values from 0.25 to 1.75
- norm_step: float32 [4096], P(('shard', 'cols')), may hold values from -0.3 to 0.3
Outputs:
- ready_gate: bfloat16 [14336, 4096], P('cols')
- ready_up: bfloat16 [14336, 4096], P('cols')
- serve_norm: bfloat16 [4096], replicated
The draws below stay inside these ranges and needn't reach their ends.
All inputs are finite; a program needn't handle non-finite values.
Results may differ from the reference program's by a relative error of at most 0.001.
Values may be sent and summed in bfloat16 or wider, within the bound.
A program may use at most 128 MiB of HBM per device.

```python
import jax
import jax.numpy as jnp

D_MODEL = 4096
D_INNER = 14336
RANK = 32


def steps_of(own_key, dims, pieces, smallest, high):
    loudness, own = 1.0, jax.random.fold_in(own_key, 6)
    for axis_at, blocks in pieces:
        draws = jnp.exp(jax.random.uniform(jax.random.fold_in(own, axis_at), (blocks,), jnp.float32, smallest / len(pieces), high / len(pieces)))
        loudness = loudness * jnp.repeat(draws, dims[axis_at] // blocks).reshape([-1 if axis == axis_at else 1 for axis in range(len(dims))])
    return loudness


def scatter_about(rng, shape, scale, bound, cuts=(), held_as=jnp.bfloat16):
    loudness = steps_of(rng, shape, cuts, -0.22, 0.18) if cuts else 1.0
    values = jax.random.normal(rng, shape, jnp.float32) * scale * loudness
    return jnp.minimum(jnp.maximum(values, -bound), bound).astype(held_as)


def setup_inputs(seed: int = 0) -> dict:
    key_list = jax.random.split(jax.random.key(seed), 9)
    return {
        "train_gate": scatter_about(key_list[0], (D_MODEL, D_INNER), D_MODEL ** -0.5, 0.09375, ((0, 4), (1, 8))),
        "low_gate": scatter_about(key_list[1], (D_MODEL, RANK), D_MODEL ** -0.5, 0.09375, ((0, 4),)),
        "high_gate": scatter_about(key_list[2], (RANK, D_INNER), RANK ** -0.5, 1.0, ((1, 8),)),
        "train_up": scatter_about(key_list[3], (D_MODEL, D_INNER), D_MODEL ** -0.5, 0.09375, ((0, 4), (1, 8))),
        "low_up": scatter_about(key_list[4], (D_MODEL, RANK), D_MODEL ** -0.5, 0.09375, ((0, 4),)),
        "high_up": scatter_about(key_list[5], (RANK, D_INNER), RANK ** -0.5, 1.0, ((1, 8),)),
        "norm_train": jnp.clip(1.0 + 0.15 * jax.random.normal(key_list[6], (D_MODEL,), jnp.float32), 0.25, 1.75),
        "norm_step": jnp.clip(jax.random.uniform(key_list[7], (D_MODEL,), jnp.float32, -0.3, 0.3) * steps_of(key_list[7], (D_MODEL,), ((0, 32),), -0.4, 0.0), -0.3, 0.3),
    }


mix_rate = 1.0


def reference(train_gate, low_gate, high_gate, train_up, low_up, high_up, norm_train, norm_step):
    latest_gate = train_gate.astype(jnp.float32) + mix_rate * jnp.dot(low_gate, high_gate, preferred_element_type=jnp.float32)
    latest_up = train_up.astype(jnp.float32) + mix_rate * jnp.dot(low_up, high_up, preferred_element_type=jnp.float32)
    ready_gate = latest_gate.T.astype(jnp.bfloat16)
    ready_up = latest_up.T.astype(jnp.bfloat16)
    serve_norm = (norm_train + norm_step).astype(jnp.bfloat16)
    return ready_gate, ready_up, serve_norm
```

```python
import functools

import jax
import jax.numpy as jnp
from jax import lax
from jax.experimental import pallas as pl
from jax.experimental.pallas import tpu as pltpu
from jax.sharding import PartitionSpec as P

mix_rate = 1.0
TILE = 256


def chunks_of(width):
    cuts, at = [], 0
    while at < width:
        size = min(TILE if at == 0 else 2 * TILE, width - at)
        cuts.append((at, size))
        at += size
    return cuts


def merge_body(train_ref, low_ref, high_ref, out_ref):
    latest = train_ref[...].astype(jnp.float32) + mix_rate * jnp.dot(
        low_ref[...], high_ref[...], preferred_element_type=jnp.float32
    )
    out_ref[...] = latest.astype(jnp.bfloat16).T


def merge(train, low, high, start, size):
    rows, rank = train.shape[0], low.shape[1]
    first = start // TILE
    return pl.pallas_call(
        merge_body,
        grid=(size // TILE,),
        in_specs=[
            pl.BlockSpec((rows, TILE), lambda j: (0, first + j)),
            pl.BlockSpec((rows, rank), lambda j: (0, 0)),
            pl.BlockSpec((rank, TILE), lambda j: (0, first + j)),
        ],
        out_specs=pl.BlockSpec((TILE, rows), lambda j: (j, 0)),
        out_shape=jax.ShapeDtypeStruct((size, rows), jnp.bfloat16),
        compiler_params=pltpu.CompilerParams(vmem_limit_bytes=16 << 20),
        cost_estimate=pl.CostEstimate(
            flops=2 * rows * rank * size, bytes_accessed=4 * rows * size, transcendentals=0
        ),
    )(train, low, high)


def place_body(cuts, flip, aliased, *refs):
    n = len(cuts)
    pieces = refs[:n]
    out = refs[n + aliased]
    bufs, get_sem, put_sem = refs[n + aliased + 1 : -2], refs[-2], refs[-1]
    me = lax.axis_index("shard")
    bit0, bit1 = lax.rem(me, 2), me // 2
    bit0 = 1 - bit0 if flip & 1 else bit0
    bit1 = 1 - bit1 if flip & 2 else bit1
    cols = pieces[0].shape[1]
    at = pl.multiple_of((bit1 * 2 + bit0) * cols, cols)
    gets, puts = [], []
    for k, (start, size) in enumerate(cuts):
        gets.append(pltpu.make_async_copy(pieces[k], bufs[k], get_sem.at[k]))
        puts.append(
            pltpu.make_async_copy(
                bufs[k], out.at[pl.ds(start, size), pl.ds(at, cols)], put_sem.at[k]
            )
        )
    for get in gets:
        get.start()
    for get, put in zip(gets, puts):
        get.wait()
        put.start()
    for put in puts:
        put.wait()


def place(out, shape, pieces, cuts, flip):
    any_spec = pl.BlockSpec(memory_space=pl.ANY)
    aliased = int(out is not None)
    n = len(pieces)
    moved = sum(2 * 2 * p.size for p in pieces)
    return pl.pallas_call(
        functools.partial(place_body, cuts, flip, aliased),
        in_specs=[any_spec] * (n + aliased),
        out_specs=any_spec,
        out_shape=jax.ShapeDtypeStruct(shape, jnp.bfloat16),
        scratch_shapes=[pltpu.VMEM(p.shape, jnp.bfloat16) for p in pieces]
        + [pltpu.SemaphoreType.DMA((n,)), pltpu.SemaphoreType.DMA((n,))],
        input_output_aliases={n: 0} if aliased else {},
        compiler_params=pltpu.CompilerParams(vmem_limit_bytes=16 << 20),
        cost_estimate=pl.CostEstimate(flops=0, bytes_accessed=moved, transcendentals=0),
    )(*pieces, *((out,) if aliased else ()))


def exchange(n, train_gate, low_gate, high_gate, train_up, low_up, high_up):
    rows, width = train_gate.shape
    cuts = chunks_of(width)
    over_x = functools.partial(lax.ppermute, axis_name="shard", perm=[(i, i ^ 1) for i in range(n)])
    over_y = functools.partial(lax.ppermute, axis_name="shard", perm=[(i, i ^ 2) for i in range(n)])
    gate, up = [], []
    for start, size in cuts:
        gate.append(merge(train_gate, low_gate, high_gate, start, size))
        up.append(merge(train_up, low_up, high_up, start, size))
    gate_x, up_y = [over_x(c) for c in gate], [over_y(c) for c in up]
    up_x, gate_y = [over_x(c) for c in up], [over_y(c) for c in gate]
    order = list(range(1, len(cuts))) + [0]
    gate_d, up_d = {}, {}
    for k in order:
        up_d[k] = over_x(up_y[k])
        gate_d[k] = over_y(gate_x[k])
    shape = (width, n * rows)
    ready = []
    for own, px, py, pd in ((gate, gate_x, gate_y, gate_d), (up, up_x, up_y, up_d)):
        out = place(None, shape, own, cuts, 0)
        first, second, fx, fy = (px, py, 1, 2) if own is gate else (py, px, 2, 1)
        out = place(out, shape, first, cuts, fx)
        out = place(out, shape, second, cuts, fy)
        for k in order:
            out = place(out, shape, [pd[k]], [cuts[k]], 3)
        ready.append(out)
    return ready


def per_device(n, train_gate, low_gate, high_gate, train_up, low_up, high_up, norm_train, norm_step):
    serve_norm = lax.all_gather(
        (norm_train + norm_step).astype(jnp.bfloat16), ("shard", "cols"), axis=0, tiled=True
    )
    rows, width = train_gate.shape
    if n == 4 and width % TILE == 0 and rows % 128 == 0:
        ready_gate, ready_up = exchange(n, train_gate, low_gate, high_gate, train_up, low_up, high_up)
    else:
        ready = []
        for train, low, high in ((train_gate, low_gate, high_gate), (train_up, low_up, high_up)):
            latest = train.astype(jnp.float32) + mix_rate * jnp.dot(
                low, high, preferred_element_type=jnp.float32
            )
            ready.append(lax.all_gather(latest.astype(jnp.bfloat16), "shard", axis=0, tiled=True).T)
        ready_gate, ready_up = ready
    return (ready_gate, ready_up, serve_norm)


def solution(mesh):
    return jax.shard_map(
        functools.partial(per_device, mesh.shape["shard"]),
        mesh=mesh,
        in_specs=(
            P("shard", "cols"),
            P("shard", None),
            P(None, "cols"),
            P("shard", "cols"),
            P("shard", None),
            P(None, "cols"),
            P(("shard", "cols")),
            P(("shard", "cols")),
        ),
        out_specs=(P("cols", None), P("cols", None), P()),
        check_vma=False,
    )
```

```python
import functools

import jax
import jax.numpy as jnp
from jax import lax
from jax.experimental import pallas as pl
from jax.experimental.pallas import tpu as pltpu
from jax.sharding import PartitionSpec as P


mix_rate = 1.0
TILE = 256
GRANT = 60 << 20


def chunks_of(width):
    cuts, at = [], 0
    while at < width:
        size = min(TILE if at == 0 else 2 * TILE, width - at)
        cuts.append((at, size))
        at += size
    return cuts


def merge_body(*refs):
    for train_ref, low_ref, high_ref, out_ref in (refs[0:3] + refs[6:7], refs[3:6] + refs[7:8]):
        update = lax.dot_general(
            low_ref[...], high_ref[...], (((0,), (0,)), ((), ())), preferred_element_type=jnp.float32
        )
        latest = train_ref[...].astype(jnp.float32) + mix_rate * update
        out_ref[...] = latest.astype(jnp.bfloat16).T


def merge(weights, start, size):
    train, low, _ = weights[0]
    rows, rank = train.shape[0], low.shape[0]
    first = start // TILE
    in_specs = [
        pl.BlockSpec((rows, TILE), lambda j: (0, first + j)),
        pl.BlockSpec((rank, rows), lambda j: (0, 0)),
        pl.BlockSpec((rank, TILE), lambda j: (0, first + j)),
    ] * 2
    return pl.pallas_call(
        merge_body,
        grid=(size // TILE,),
        in_specs=in_specs,
        out_specs=[pl.BlockSpec((TILE, rows), lambda j: (j, 0))] * 2,
        out_shape=[jax.ShapeDtypeStruct((size, rows), jnp.bfloat16)] * 2,
        compiler_params=pltpu.CompilerParams(vmem_limit_bytes=GRANT),
        cost_estimate=pl.CostEstimate(
            flops=4 * rows * rank * size, bytes_accessed=8 * rows * size, transcendentals=0
        ),
    )(*weights[0], *weights[1])


def place_body(jobs, aliased, *refs):
    n = len(jobs)
    pieces, outs = refs[:n], refs[n + aliased : n + aliased + 2]
    bufs, get_sem, put_sem = refs[n + aliased + 2 : -2], refs[-2], refs[-1]
    me = lax.axis_index("shard")
    bit0, bit1 = lax.rem(me, 2), me // 2
    gets, puts = [], []
    for k, (which, start, size, flip) in enumerate(jobs):
        cols = pieces[k].shape[1]
        source = (1 - bit1 if flip & 2 else bit1) * 2 + (1 - bit0 if flip & 1 else bit0)
        at = pl.multiple_of(source * cols, cols)
        gets.append(pltpu.make_async_copy(pieces[k], bufs[k], get_sem.at[k]))
        puts.append(
            pltpu.make_async_copy(
                bufs[k], outs[which].at[pl.ds(start, size), pl.ds(at, cols)], put_sem.at[k]
            )
        )
    for get in gets:
        get.start()
    for get, put in zip(gets, puts):
        get.wait()
        put.start()
    for put in puts:
        put.wait()


def place(outs, shape, pieces, jobs):
    any_spec = pl.BlockSpec(memory_space=pl.ANY)
    aliased = len(outs)
    n = len(pieces)
    moved = sum(2 * 2 * p.size for p in pieces)
    return pl.pallas_call(
        functools.partial(place_body, jobs, aliased),
        in_specs=[any_spec] * (n + aliased),
        out_specs=[any_spec] * 2,
        out_shape=[jax.ShapeDtypeStruct(shape, jnp.bfloat16)] * 2,
        scratch_shapes=[pltpu.VMEM(p.shape, jnp.bfloat16) for p in pieces]
        + [pltpu.SemaphoreType.DMA((n,)), pltpu.SemaphoreType.DMA((n,))],
        input_output_aliases={n: 0, n + 1: 1} if aliased else {},
        compiler_params=pltpu.CompilerParams(vmem_limit_bytes=GRANT),
        cost_estimate=pl.CostEstimate(flops=0, bytes_accessed=moved, transcendentals=0),
    )(*pieces, *outs)


def last_order(cuts):
    return list(range(1, len(cuts))) + [0]


def hop(n, step, piece):
    return lax.ppermute(piece, "shard", perm=[(i, i ^ step) for i in range(n)])


def exchange(n, weights):
    rows, width = weights[0][0].shape
    cuts = chunks_of(width)
    span = range(len(cuts))
    gate, up = [], []
    for k in span:
        g, u = merge(weights, *cuts[k])
        gate.append(g)
        up.append(u)
    gate_x = [hop(n, 1, gate[k]) for k in span]
    up_y = [hop(n, 2, up[k]) for k in span]
    up_x = [hop(n, 1, up[k]) for k in span]
    gate_y = [hop(n, 2, gate[k]) for k in span]
    up_d = [hop(n, 1, up_y[k]) for k in span]
    gate_d = [hop(n, 2, gate_x[k]) for k in span]
    stages = [
        [(gate[k], (0, *cuts[k], 0)) for k in span] + [(up[k], (1, *cuts[k], 0)) for k in span],
        [p for k in span for p in ((gate_x[k], (0, *cuts[k], 1)), (up_y[k], (1, *cuts[k], 2)))],
        [p for k in span for p in ((gate_y[k], (0, *cuts[k], 2)), (up_x[k], (1, *cuts[k], 1)))],
    ]
    for k in last_order(cuts):
        stages.append([(gate_d[k], (0, *cuts[k], 3)), (up_d[k], (1, *cuts[k], 3))])
    outs = ()
    for stage in stages:
        outs = place(outs, (width, n * rows), [p for p, _ in stage], tuple(j for _, j in stage))
    return outs


def fits(n, rows, width):
    return n == 4 and width % TILE == 0 and rows % 128 == 0


def per_device(n, train_gate, low_gate, high_gate, train_up, low_up, high_up, norm_train, norm_step):
    serve_norm = lax.all_gather((norm_train + norm_step).astype(jnp.bfloat16), ("shard", "cols"), axis=0, tiled=True)
    if fits(n, *train_gate.shape):
        ready_gate, ready_up = exchange(
            n, ((train_gate, low_gate.T, high_gate), (train_up, low_up.T, high_up))
        )
    else:
        ready = []
        for train, low, high in ((train_gate, low_gate, high_gate), (train_up, low_up, high_up)):
            latest = train.astype(jnp.float32) + mix_rate * jnp.dot(
                low, high, preferred_element_type=jnp.float32
            )
            ready.append(lax.all_gather(latest.astype(jnp.bfloat16), "shard", axis=0, tiled=True).T)
        ready_gate, ready_up = ready
    return (ready_gate, ready_up, serve_norm)


def solution(mesh):
    n = mesh.shape["shard"]
    step = jax.shard_map(
        functools.partial(per_device, n),
        mesh=mesh,
        in_specs=(
            P("shard", "cols"),
            P("shard", None),
            P(None, "cols"),
            P("shard", "cols"),
            P("shard", None),
            P(None, "cols"),
            P(("shard", "cols")),
            P(("shard", "cols")),
        ),
        out_specs=(P("cols", None), P("cols", None), P()),
        check_vma=False,
    )

    def whole(train_gate, *rest):
        rows, width = train_gate.shape[0] // n, train_gate.shape[1] // mesh.shape["cols"]
        run = step
        if fits(n, rows, width):
            run = step
        return run(train_gate, *rest)

    return whole
```

```python
import functools

import jax
import jax.numpy as jnp
from jax import lax
from jax.experimental import pallas as pl
from jax.experimental.pallas import tpu as pltpu
from jax.sharding import PartitionSpec as P


mix_rate = 1.0
TILE = 128
GRANT = 60 << 20
GROWTH = {1: 3, 3: 4}


def chunks_of(width):
    cuts, at, tiles = [], 0, 1
    while at < width:
        size = min(tiles * TILE, width - at)
        cuts.append((at, size))
        at += size
        tiles = GROWTH.get(tiles, 6)
    return cuts


def merge_body(*refs):
    for train_ref, low_ref, high_ref, out_ref in (refs[0:3] + refs[6:7], refs[3:6] + refs[7:8]):
        update = lax.dot_general(
            low_ref[...], high_ref[...], (((0,), (0,)), ((), ())), preferred_element_type=jnp.float32
        )
        latest = train_ref[...].astype(jnp.float32) + mix_rate * update
        out_ref[...] = latest.astype(jnp.bfloat16).T


def merge(weights, start, size):
    train, low, _ = weights[0]
    rows, rank = train.shape[0], low.shape[0]
    tile = 2 * TILE if start % (2 * TILE) == 0 and size % (2 * TILE) == 0 else TILE
    first = start // tile
    in_specs = [
        pl.BlockSpec((rows, tile), lambda j: (0, first + j)),
        pl.BlockSpec((rank, rows), lambda j: (0, 0)),
        pl.BlockSpec((rank, tile), lambda j: (0, first + j)),
    ] * 2
    return pl.pallas_call(
        merge_body,
        grid=(size // tile,),
        in_specs=in_specs,
        out_specs=[pl.BlockSpec((tile, rows), lambda j: (j, 0))] * 2,
        out_shape=[jax.ShapeDtypeStruct((size, rows), jnp.bfloat16)] * 2,
        compiler_params=pltpu.CompilerParams(vmem_limit_bytes=GRANT),
        cost_estimate=pl.CostEstimate(
            flops=4 * rows * rank * size, bytes_accessed=8 * rows * size, transcendentals=0
        ),
    )(*weights[0], *weights[1])


def place_body(jobs, aliased, *refs):
    n = len(jobs)
    pieces, outs = refs[:n], refs[n + aliased : n + aliased + 2]
    bufs, get_sem, put_sem = refs[n + aliased + 2 : -2], refs[-2], refs[-1]
    me = lax.axis_index("shard")
    bit0, bit1 = lax.rem(me, 2), me // 2
    gets, puts = [], []
    for k, (which, start, size, flip) in enumerate(jobs):
        cols = pieces[k].shape[1]
        source = (1 - bit1 if flip & 2 else bit1) * 2 + (1 - bit0 if flip & 1 else bit0)
        at = pl.multiple_of(source * cols, cols)
        gets.append(pltpu.make_async_copy(pieces[k], bufs[k], get_sem.at[k]))
        puts.append(
            pltpu.make_async_copy(
                bufs[k], outs[which].at[pl.ds(start, size), pl.ds(at, cols)], put_sem.at[k]
            )
        )
    for get in gets:
        get.start()
    for get, put in zip(gets, puts):
        get.wait()
        put.start()
    for put in puts:
        put.wait()


def place(outs, shape, pieces, jobs):
    any_spec = pl.BlockSpec(memory_space=pl.ANY)
    aliased = len(outs)
    n = len(pieces)
    moved = sum(2 * 2 * p.size for p in pieces)
    return pl.pallas_call(
        functools.partial(place_body, jobs, aliased),
        in_specs=[any_spec] * (n + aliased),
        out_specs=[any_spec] * 2,
        out_shape=[jax.ShapeDtypeStruct(shape, jnp.bfloat16)] * 2,
        scratch_shapes=[pltpu.VMEM(p.shape, jnp.bfloat16) for p in pieces]
        + [pltpu.SemaphoreType.DMA((n,)), pltpu.SemaphoreType.DMA((n,))],
        input_output_aliases={n: 0, n + 1: 1} if aliased else {},
        compiler_params=pltpu.CompilerParams(vmem_limit_bytes=GRANT),
        cost_estimate=pl.CostEstimate(flops=0, bytes_accessed=moved, transcendentals=0),
    )(*pieces, *outs)


def last_order(cuts):
    return list(range(len(cuts)))[::-1]


def hop(n, step, piece):
    return lax.ppermute(piece, "shard", perm=[(i, i ^ step) for i in range(n)])


def exchange(n, weights):
    rows, width = weights[0][0].shape
    cuts = chunks_of(width)
    span = range(len(cuts))
    gate, up = [], []
    for k in span:
        g, u = merge(weights, *cuts[k])
        gate.append(g)
        up.append(u)
    gate_x = [hop(n, 1, gate[k]) for k in span]
    up_y = [hop(n, 2, up[k]) for k in span]
    up_x = [hop(n, 1, up[k]) for k in span]
    gate_y = [hop(n, 2, gate[k]) for k in span]
    up_d = [hop(n, 1, up_y[k]) for k in span]
    gate_d = [hop(n, 2, gate_x[k]) for k in span]
    stages = [
        [(gate[k], (0, *cuts[k], 0)) for k in span] + [(up[k], (1, *cuts[k], 0)) for k in span],
        [p for k in span for p in ((gate_x[k], (0, *cuts[k], 1)), (up_y[k], (1, *cuts[k], 2)))],
        [p for k in span for p in ((gate_y[k], (0, *cuts[k], 2)), (up_x[k], (1, *cuts[k], 1)))],
    ]
    for k in last_order(cuts):
        stages.append([(gate_d[k], (0, *cuts[k], 3)), (up_d[k], (1, *cuts[k], 3))])
    outs = ()
    for stage in stages:
        outs = place(outs, (width, n * rows), [p for p, _ in stage], tuple(j for _, j in stage))
    return outs


def fits(n, rows, width):
    return n == 4 and width % TILE == 0 and rows % 128 == 0


def per_device(n, train_gate, low_gate, high_gate, train_up, low_up, high_up, norm_train, norm_step):
    serve_norm = lax.all_gather((norm_train + norm_step).astype(jnp.bfloat16), ("shard", "cols"), axis=0, tiled=True)
    if fits(n, *train_gate.shape):
        ready_gate, ready_up = exchange(
            n, ((train_gate, low_gate.T, high_gate), (train_up, low_up.T, high_up))
        )
    else:
        ready = []
        for train, low, high in ((train_gate, low_gate, high_gate), (train_up, low_up, high_up)):
            latest = train.astype(jnp.float32) + mix_rate * jnp.dot(
                low, high, preferred_element_type=jnp.float32
            )
            ready.append(lax.all_gather(latest.astype(jnp.bfloat16), "shard", axis=0, tiled=True).T)
        ready_gate, ready_up = ready
    return (ready_gate, ready_up, serve_norm)


def solution(mesh):
    n = mesh.shape["shard"]
    step = jax.shard_map(
        functools.partial(per_device, n),
        mesh=mesh,
        in_specs=(
            P("shard", "cols"),
            P("shard", None),
            P(None, "cols"),
            P("shard", "cols"),
            P("shard", None),
            P(None, "cols"),
            P(("shard", "cols")),
            P(("shard", "cols")),
        ),
        out_specs=(P("cols", None), P("cols", None), P()),
        check_vma=False,
    )

    def whole(train_gate, *rest):
        rows, width = train_gate.shape[0] // n, train_gate.shape[1] // mesh.shape["cols"]
        run = step
        if fits(n, rows, width):
            run = step
        return run(train_gate, *rest)

    return whole
```
